32 devices in a mesh: shard: 8 (over y, x, core), tp: 4 (over z).
Axes of the slice: x: 2, y: 2, z: 4, core: 2. Of those that a mesh axis runs over, the one named last changes fastest.
Arguments:
- train_query: bfloat16 [5120, 8192], P('shard', 'tp'), may hold values from -0.078125 to 0.078125
- low_query: bfloat16 [5120, 32], P('shard'), may hold values from -0.078125 to 0.078125
- high_query: bfloat16 [32, 8192], P(None, 'tp'), may hold values from -1 to 1
- train_key: bfloat16 [5120, 1024], P('shard', 'tp'), may hold values from -0.078125 to 0.078125
- low_key: bfloat16 [5120, 32], P('shard'), may hold values from -0.078125 to 0.078125
- high_key: bfloat16 [32, 1024], P(None, 'tp'), may hold values from -1 to 1
- train_value: bfloat16 [5120, 1024], P('shard', 'tp'), may hold values from -0.078125 to 0.078125
- low_value: bfloat16 [5120, 32], P('shard'), may hold values from -0.078125 to 0.078125
- high_value: bfloat16 [32, 1024], P(None, 'tp'), may hold values from -1 to 1
- train_mixed: bfloat16 [8192, 5120], P('tp', 'shard'), may hold values from -0.0625 to 0.0625
- low_mixed: bfloat16 [8192, 32], P('tp'), may hold values from -0.0625 to 0.0625
- high_mixed: bfloat16 [32, 5120], P(None, 'shard'), may hold values from -1 to 1
- norm_train: float32 [5120], P(('shard', 'tp')), may hold values from 0.25 to 1.75
- norm_step: float32 [5120], P(('shard', 'tp')), may hold values from -0.3 to 0.3
Outputs:
- final_query: bfloat16 [5120, 8192], P(None, 'tp')
- final_key: bfloat16 [5120, 1024], P(None, 'tp')
- final_value: bfloat16 [5120, 1024], P(None, 'tp')
- final_mixed: bfloat16 [8192, 5120], P('tp')
- serve_norm: bfloat16 [5120], replicated
The draws below stay inside these ranges and needn't reach their ends.
All inputs are finite; a program needn't handle non-finite values.
Results may differ from the reference program's by a relative error of at most 0.001.
Values may be sent and summed in bfloat16 or wider, within the bound.
No kernel may reach another device: no remote copies, remote signals or barrier semaphores. Data moves between devices by JAX's collectives and lax.ppermute only.
A program may use at most 192 MiB of HBM per device.

```python
import jax
import jax.numpy as jnp

D_MODEL = 5120
Q_DIM = 8192
KV_DIM = 1024
RANK = 32


def block_scale(rng, shape, shards, low, top_value):
    gain = 1.0
    for position, parts in shards:
        steps = jax.random.uniform(jax.random.fold_in(jax.random.fold_in(rng, 6), position), (parts,), jnp.float32, low / len(shards), top_value / len(shards))
        gain = gain * jnp.repeat(jnp.exp(steps), shape[position] // parts).reshape((-1,) + (1,) * (len(shape) - 1 - position))
    return gain


def noise(rng, extent, width, bound, split=(), held_as=jnp.bfloat16):
    values = width * jax.random.normal(rng, extent, jnp.float32)
    if split:
        values = values * block_scale(rng, extent, split, -0.22, 0.18)
    return jnp.clip(values, -bound, bound).astype(held_as)


def setup_inputs(seed: int = 0) -> dict:
    key_list = jax.random.split(jax.random.key(seed), 15)
    return {
        "train_query": noise(key_list[0], (D_MODEL, Q_DIM), D_MODEL ** -0.5, 0.078125, ((0, 8), (1, 4))),
        "low_query": noise(key_list[1], (D_MODEL, RANK), D_MODEL ** -0.5, 0.078125, ((0, 8),)),
        "high_query": noise(key_list[2], (RANK, Q_DIM), RANK ** -0.5, 1.0, ((1, 4),)),
        "train_key": noise(key_list[3], (D_MODEL, KV_DIM), D_MODEL ** -0.5, 0.078125, ((0, 8), (1, 4))),
        "low_key": noise(key_list[4], (D_MODEL, RANK), D_MODEL ** -0.5, 0.078125, ((0, 8),)),
        "high_key": noise(key_list[5], (RANK, KV_DIM), RANK ** -0.5, 1.0, ((1, 4),)),
        "train_value": noise(key_list[6], (D_MODEL, KV_DIM), D_MODEL ** -0.5, 0.078125, ((0, 8), (1, 4))),
        "low_value": noise(key_list[7], (D_MODEL, RANK), D_MODEL ** -0.5, 0.078125, ((0, 8),)),
        "high_value": noise(key_list[8], (RANK, KV_DIM), RANK ** -0.5, 1.0, ((1, 4),)),
        "train_mixed": noise(key_list[9], (Q_DIM, D_MODEL), Q_DIM ** -0.5, 0.0625, ((0, 4), (1, 8))),
        "low_mixed": noise(key_list[10], (Q_DIM, RANK), Q_DIM ** -0.5, 0.0625, ((0, 4),)),
        "high_mixed": noise(key_list[11], (RANK, D_MODEL), RANK ** -0.5, 1.0, ((1, 8),)),
        "norm_train": jnp.clip(1.0 + 0.15 * jax.random.normal(key_list[12], (D_MODEL,), jnp.float32), 0.25, 1.75),
        "norm_step": jnp.clip(jax.random.uniform(key_list[13], (D_MODEL,), jnp.float32, -0.3, 0.3) * block_scale(key_list[13], (D_MODEL,), ((0, 32),), -0.4, 0.0), -0.3, 0.3),
    }


mix_rate = 0.5


def reference(train_query, low_query, high_query, train_key, low_key, high_key, train_value, low_value, high_value, train_mixed, low_mixed, high_mixed, norm_train, norm_step):
    result_query = train_query.astype(jnp.float32) + mix_rate * jnp.dot(low_query, high_query, preferred_element_type=jnp.float32)
    result_key = train_key.astype(jnp.float32) + mix_rate * jnp.dot(low_key, high_key, preferred_element_type=jnp.float32)
    result_value = train_value.astype(jnp.float32) + mix_rate * jnp.dot(low_value, high_value, preferred_element_type=jnp.float32)
    result_mixed = train_mixed.astype(jnp.float32) + mix_rate * jnp.dot(low_mixed, high_mixed, preferred_element_type=jnp.float32)
    final_query = result_query.astype(jnp.bfloat16)
    final_key = result_key.astype(jnp.bfloat16)
    final_value = result_value.astype(jnp.bfloat16)
    final_mixed = result_mixed.astype(jnp.bfloat16)
    serve_norm = (norm_train + norm_step).astype(jnp.bfloat16)
    return final_query, final_key, final_value, final_mixed, serve_norm
```

```python
import jax
import jax.numpy as jnp
from jax import lax
from jax.sharding import PartitionSpec as P

mix_rate = 0.5
CORES = 2


def merge(train, low, high):
    result = train.astype(jnp.float32) + mix_rate * jnp.dot(
        low, high, preferred_element_type=jnp.float32
    )
    return result.astype(jnp.bfloat16)


def ring_of(chips):
    width = chips // 2 if chips % 2 == 0 else chips
    return list(range(width)) + list(range(chips - 1, width - 1, -1))


def build(shard, tp):
    chips = shard // CORES
    ring = ring_of(chips)
    place = [ring.index(chip) for chip in range(chips)]

    def hop(by):
        return [
            (chip * CORES + core, ring[(place[chip] + by) % chips] * CORES + core)
            for chip in range(chips)
            for core in range(CORES)
        ]

    right, left = hop(1), hop(-1)
    swap = [(i, i ^ 1) for i in range(shard)]

    def body(
        train_query,
        low_query,
        high_query,
        train_key,
        low_key,
        high_key,
        train_value,
        low_value,
        high_value,
        train_mixed,
        low_mixed,
        high_mixed,
        norm_train,
        norm_step,
    ):
        me = lax.axis_index("shard")
        chip, core = me // CORES, me % CORES
        width = ring.index(chips - 1)

        def to_place(c):
            return jnp.where(c < width, c, chips - 1 + width - c)

        at = to_place(chip)

        def source(by):
            return to_place((at + chips - by) % chips) * CORES + core

        own = {
            "k": merge(train_key, low_key, high_key),
            "v": merge(train_value, low_value, high_value),
            "q": merge(train_query, low_query, high_query),
            "m": merge(train_mixed, low_mixed, high_mixed),
        }
        dims = {"q": 0, "k": 0, "v": 0, "m": 1}
        out = {}
        for name, block in own.items():
            shape = list(block.shape)
            shape[dims[name]] *= shard
            out[name] = jnp.zeros(shape, block.dtype)

        def put(name, block, owner):
            starts = [0, 0]
            starts[dims[name]] = owner * block.shape[dims[name]]
            out[name] = lax.dynamic_update_slice(out[name], block, starts)

        def arrive(name, block, owner):
            put(name, block, owner)
            put(name, lax.ppermute(block, "shard", swap), owner ^ 1)

        for name in own:
            arrive(name, own[name], me)

        going_right = dict(own)
        going_left = dict(own)
        for by in range(1, chips // 2 + 1):
            last = 2 * by == chips
            for name in ("k", "q") if last else ("k", "q", "m", "v"):
                going_right[name] = lax.ppermute(going_right[name], "shard", right)
            for name in ("v", "m") if last else ("v", "m", "q", "k"):
                going_left[name] = lax.ppermute(going_left[name], "shard", left)
            for name in ("k", "q") if last else ("k", "q", "m", "v"):
                arrive(name, going_right[name], source(by))
            for name in ("v", "m") if last else ("v", "m", "q", "k"):
                arrive(name, going_left[name], source(-by))

        step = (norm_train + norm_step).astype(jnp.bfloat16)
        parts = step[None, :]
        column = lax.axis_index("tp")
        norm = jnp.zeros((tp, step.shape[0]), step.dtype)
        norm = lax.dynamic_update_slice(norm, parts, (column, 0))
        for by in range(1, tp):
            moved = lax.ppermute(parts, "tp", [(i, (i + by) % tp) for i in range(tp)])
            norm = lax.dynamic_update_slice(norm, moved, ((column + tp - by) % tp, 0))
        norm = norm.reshape(1, -1)
        serve = jnp.zeros((shard, norm.shape[1]), norm.dtype)
        serve = lax.dynamic_update_slice(serve, norm, (me, 0))
        for by in range(1, shard):
            moved = lax.ppermute(norm, "shard", [(i, (i + by) % shard) for i in range(shard)])
            serve = lax.dynamic_update_slice(serve, moved, ((me + shard - by) % shard, 0))
        return out["q"], out["k"], out["v"], out["m"], serve.reshape(-1)

    return body


def solution(mesh):
    return jax.shard_map(
        build(mesh.shape["shard"], mesh.shape["tp"]),
        mesh=mesh,
        in_specs=(
            P("shard", "tp"),
            P("shard", None),
            P(None, "tp"),
            P("shard", "tp"),
            P("shard", None),
            P(None, "tp"),
            P("shard", "tp"),
            P("shard", None),
            P(None, "tp"),
            P("tp", "shard"),
            P("tp", None),
            P(None, "shard"),
            P(("shard", "tp")),
            P(("shard", "tp")),
        ),
        out_specs=(P(None, "tp"), P(None, "tp"), P(None, "tp"), P("tp", None), P()),
        check_vma=False,
    )
```
